16 devices in a mesh: dp: 4 (over y, z), tp: 4 (over x, core).
Axes of the slice: x: 2, y: 2, z: 2, core: 2. Of those that a mesh axis runs over, the one named last changes fastest.
Arguments:
- x: bfloat16 [4, 2048, 1024], P('dp', 'tp')
- dy: bfloat16 [4, 2048, 1024], P('dp', 'tp')
- wq: bfloat16 [1024, 4096], P('dp', 'tp')
- wk: bfloat16 [1024, 4096], P('dp', 'tp')
- wv: bfloat16 [1024, 4096], P('dp', 'tp')
- wo: bfloat16 [4096, 1024], P(('tp', 'dp'))
- w_gate: bfloat16 [1024, 16384], P('dp', 'tp')
- w_up: bfloat16 [1024, 16384], P('dp', 'tp')
- w_down: bfloat16 [16384, 1024], P(('tp', 'dp'))
Outputs:
- output 1: bfloat16 [4, 2048, 1024], P('dp', 'tp')
- output 2: bfloat16 [1024, 4096], P('dp', 'tp')
- output 3: bfloat16 [1024, 4096], P('dp', 'tp')
- output 4: bfloat16 [1024, 4096], P('dp', 'tp')
- output 5: bfloat16 [4096, 1024], P(('tp', 'dp'))
- output 6: bfloat16 [1024, 16384], P('dp', 'tp')
- output 7: bfloat16 [1024, 16384], P('dp', 'tp')
- output 8: bfloat16 [16384, 1024], P(('tp', 'dp'))
All inputs are finite; a program needn't handle non-finite values.
Results may differ from the reference program's by a relative error of at most 0.024.
Values are sent between devices in bfloat16 or wider.
A program may use at most 2 GiB of HBM per device.

```python
import jax
import jax.numpy as jnp
from jax import lax

SEQUENCES = 4
TOKENS = 2048
D = 1024
HEADS = 32
KV_HEADS = 32
HEAD = 128
FF = 16384
THETA = 10000
NAMES = ("wq", "wk", "wv", "wo", "w_gate", "w_up", "w_down")
SHAPES = {
    "wq": (D, HEADS * HEAD),
    "wk": (D, KV_HEADS * HEAD),
    "wv": (D, KV_HEADS * HEAD),
    "wo": (HEADS * HEAD, D),
    "w_gate": (D, FF),
    "w_up": (D, FF),
    "w_down": (FF, D),
}


def bump(key, n, height):
    away = (jnp.arange(n, dtype=jnp.int32) - jax.random.randint(key, (), 0, n, jnp.int32)) % n
    return jnp.where(away < n // 8, height, 1.0)


def together(key, own, strength):
    shared = jax.random.normal(key, own.shape[1:], jnp.float32)
    return (own + strength * shared) * lax.rsqrt(1 + strength * strength)


def setup_inputs(seed: int = 0, part: int = 0) -> dict:
    kx, kdy, ka, kb, kz, kf, kh, kl, *kw = jax.random.split(jax.random.key(seed), 8 + len(NAMES))
    shape = (SEQUENCES, TOKENS, D)
    much_x, much_dy = jax.random.uniform(kz, (2,), jnp.float32, 0.0, 1.0)
    loud = 2.0 ** jax.random.uniform(jax.random.fold_in(kz, 1), (), jnp.float32, -1.0, 2.0)
    halves = 2.0 ** jax.random.uniform(kl, (2,), jnp.float32, -1.0, 1.0)
    times = {"wq": 1.0, "wk": 1.0, "wv": 2.0, "wo": halves[0], "w_gate": 1.0, "w_up": bump(kh, FF, 4.0), "w_down": halves[1]}
    x = together(ka, jax.random.normal(kx, shape, jnp.float32), much_x) * bump(kf, D, 4.0)
    dy = together(kb, jax.random.normal(kdy, shape, jnp.float32), much_dy)
    drawn = {"x": x.astype(jnp.bfloat16), "dy": (loud * dy * (SEQUENCES * TOKENS) ** -0.5).astype(jnp.bfloat16)}
    for key, name in zip(kw, NAMES, strict=True):
        drawn[name] = (jax.random.normal(key, SHAPES[name], jnp.float32) * SHAPES[name][0] ** -0.5 * times[name]).astype(jnp.bfloat16)
    return drawn


def matmul(a, w):
    return jnp.dot(a, w, preferred_element_type=jnp.float32).astype(jnp.bfloat16)


def normed(h):
    wide = h.astype(jnp.float32)
    scale = lax.rsqrt(jnp.mean(wide**2, -1, keepdims=True) + 1e-6)
    return (wide * scale).astype(jnp.bfloat16)


def turned(t, theta):
    half = t.shape[-1] // 2
    angle = jnp.arange(t.shape[0], dtype=jnp.float32)[:, None] * theta ** (-jnp.arange(half, dtype=jnp.float32) / half)
    cos, sin = jnp.cos(angle)[:, None], jnp.sin(angle)[:, None]
    a, b = t[..., :half].astype(jnp.float32), t[..., half:].astype(jnp.float32)
    return jnp.concatenate([a * cos - b * sin, b * cos + a * sin], -1).astype(jnp.bfloat16)


def seen_by(q, k, v):
    tokens, kv = q.shape[0], k.shape[1]
    q = q.reshape(tokens, kv, -1, q.shape[-1])
    scores = jnp.einsum("tgsd,ugd->gstu", q.astype(jnp.float32), k.astype(jnp.float32)) * q.shape[-1] ** -0.5
    place = jnp.arange(tokens)
    weights = jax.nn.softmax(jnp.where(place[:, None] >= place, scores, -jnp.inf), -1).astype(jnp.bfloat16)
    return jnp.einsum("gstu,ugd->tgsd", weights.astype(jnp.float32), v.astype(jnp.float32)).astype(jnp.bfloat16).reshape(tokens, -1)


def layer(h, w):
    a = normed(h)
    q, k = (turned(matmul(a, w[name]).reshape(h.shape[0], -1, HEAD), THETA) for name in ("wq", "wk"))
    h = h + matmul(seen_by(q, k, matmul(a, w["wv"]).reshape(h.shape[0], -1, HEAD)), w["wo"])
    b = normed(h)
    gate = jnp.dot(b, w["w_gate"], preferred_element_type=jnp.float32)
    up = jnp.dot(b, w["w_up"], preferred_element_type=jnp.float32)
    return h + matmul((jax.nn.silu(gate) * up).astype(jnp.bfloat16), w["w_down"])


def reference(x, dy, wq, wk, wv, wo, w_gate, w_up, w_down):
    weights = dict(zip(NAMES, (wq, wk, wv, wo, w_gate, w_up, w_down), strict=True))

    def take(so_far, sequence):
        h, by_y = sequence
        _, back = jax.vjp(lambda w, h: layer(h, w), weights, h)
        by_weights, by_h = back(by_y)
        return jax.tree.map(lambda total, term: total + term.astype(jnp.float32), so_far, by_weights), by_h

    none_yet = {name: jnp.zeros(w.shape, jnp.float32) for name, w in weights.items()}
    by_weights, by_x = lax.scan(take, none_yet, (x, dy))
    return (by_x, *(by_weights[name].astype(jnp.bfloat16) for name in NAMES))
```

```python
import jax
import jax.numpy as jnp
from jax import lax
from jax.experimental import pallas as pl
from jax.experimental.pallas import tpu as pltpu
from jax.sharding import PartitionSpec as P


F32, BF16 = jnp.float32, jnp.bfloat16
NEG = -1e30
HIDDEN = 2 * NEG
LOG2E = 1.4426950408889634
VMEM = 44 * 2**20
HEAD = 128
HEADS = 8
SCALE = HEAD**-0.5
THETA = 10000
D = 1024
SEQ = 2048
ROWS = 256
CHUNK = 512
PART = 4 * HEAD
ORDER = (0, 2, 3, 1)


def _dot(a, b, ca, cb):
    return lax.dot_general(a, b, (((ca,), (cb,)), ((), ())), preferred_element_type=F32)


def shape(*dims, dtype=BF16):
    return jax.ShapeDtypeStruct(dims, dtype)


def whole(*dims):
    return pl.BlockSpec(dims, lambda *_: (0,) * len(dims), pipeline_mode=pl.Buffered(1))


def rows(width, first=0, column=0):
    return pl.BlockSpec((CHUNK, width), lambda i, s: (first + i, column))


def call(body, s, steps, args, in_specs, outs, out_specs, flops, aliases=None, scratch=()):
    cost = pl.CostEstimate(flops=flops, transcendentals=0, bytes_accessed=sum(a.size * a.dtype.itemsize for a in (*args, *outs)))
    return pl.pallas_call(
        body,
        grid_spec=pltpu.PrefetchScalarGridSpec(num_scalar_prefetch=1, grid=(steps,), in_specs=in_specs, out_specs=out_specs, scratch_shapes=scratch),
        out_shape=outs,
        input_output_aliases=aliases or {},
        compiler_params=pltpu.CompilerParams(dimension_semantics=("arbitrary",), vmem_limit_bytes=VMEM),
        cost_estimate=cost,
    )(s, *args)


def place(d, k):
    return pl.ds(pl.multiple_of((d ^ k) * ROWS, ROWS), ROWS)


def total(terms):
    acc = None
    for term in terms:
        acc = term if acc is None else acc + term
    return acc


def pick(refs, into):
    for c, ref in enumerate(refs):

        @pl.when(pl.program_id(0) == c)
        def _():
            into[...] = ref[...]


def sort(value, keep_ref, give_ref):
    @pl.when(pl.program_id(0) % 2 == 0)
    def _():
        keep_ref[...] = value

    @pl.when(pl.program_id(0) % 2 == 1)
    def _():
        give_ref[...] = value


def across(first=0):
    return pl.BlockSpec((D, CHUNK), lambda i, s: (0, first + i))


CHUNKED = pltpu.VMEM((CHUNK, D), BF16)
TURNS = pl.BlockSpec((CHUNK, D), lambda i, s: (i // 2, 0))


def attend(s, q, k, v):
    e = SCALE * LOG2E

    def body(s_ref, q_ref, k_ref, v_ref, o_ref, lse_ref, top_s, mix_s):
        iq = pl.program_id(0)
        top_s[...] = jnp.full_like(top_s, NEG)
        mix_s[...] = jnp.zeros_like(mix_s)
        ones = jnp.ones((8, CHUNK), BF16)

        def block(j, masked):
            here = pl.ds(pl.multiple_of(j * CHUNK, CHUNK), CHUNK)
            scores = [_dot(k_ref[i, here, :], q_ref[i], 1, 1) for i in range(HEADS)]
            weights, keeps = [], []
            for i, score in enumerate(scores):
                if masked:
                    seen = lax.broadcasted_iota(jnp.int32, score.shape, 1) >= lax.broadcasted_iota(jnp.int32, score.shape, 0)
                    score = jnp.where(seen, score, HIDDEN)
                old = top_s[i]
                top = jnp.maximum(old, score.max(axis=0, keepdims=True))
                top_s[i] = top
                weights.append(jnp.exp2((score - top) * e).astype(BF16))
                keeps.append(jnp.exp2((old - top) * e))
            for i, (p, keep) in enumerate(zip(weights, keeps)):
                values = jnp.concatenate([v_ref[i, here, :].T, ones], axis=0)
                mix_s[i] = mix_s[i] * keep + _dot(values, p, 1, 0)

        lax.fori_loop(0, iq, lambda j, _: block(j, False), None)
        block(iq, True)
        for i in range(HEADS):
            amount = mix_s[i, HEAD : HEAD + 1, :]
            o_ref[i] = (mix_s[i, :HEAD, :] * (1 / amount)).T.astype(BF16)
            lse_ref[i] = top_s[i] * SCALE + jnp.log(amount)

    queries = pl.BlockSpec((HEADS, CHUNK, HEAD), lambda i, s: (0, i, 0))
    keys = whole(HEADS, SEQ, HEAD)
    return call(body, s, SEQ // CHUNK, (q, k, v), [queries, keys, keys], [shape(HEADS, SEQ, HEAD), shape(HEADS, 1, SEQ, dtype=F32)],
                [queries, pl.BlockSpec((HEADS, 1, CHUNK), lambda i, s: (0, 0, i))], 2 * HEADS * SEQ * SEQ * HEAD,
                scratch=[pltpu.VMEM((HEADS, 1, CHUNK), F32), pltpu.VMEM((HEADS, HEAD + 8, CHUNK), F32)])


def attend_back(s, q, k, v, do, lse, delta, cos, sin, first):
    few = HEADS // 2
    e = SCALE * LOG2E

    def body(s_ref, q_ref, k_ref, v_ref, do_ref, lse_ref, delta_ref, cos_ref, sin_ref, g_ref, dq_s, dk_s, dv_s):
        iq = pl.program_id(0)

        @pl.when(iq == 0)
        def _():
            dk_s[...] = jnp.zeros_like(dk_s)
            dv_s[...] = jnp.zeros_like(dv_s)

        dq_s[...] = jnp.zeros_like(dq_s)

        def block(j, masked):
            here = pl.ds(pl.multiple_of(j * CHUNK, CHUNK), CHUNK)
            scores = [_dot(k_ref[i, here, :], q_ref[i], 1, 1) for i in range(few)]
            dps = [_dot(v_ref[i, here, :], do_ref[i], 1, 1) for i in range(few)]
            for i in range(few):
                p = jnp.exp2(scores[i] * e - lse_ref[i] * LOG2E)
                if masked:
                    seen = lax.broadcasted_iota(jnp.int32, p.shape, 1) >= lax.broadcasted_iota(jnp.int32, p.shape, 0)
                    p = jnp.where(seen, p, 0.0)
                ds = (p * (dps[i] - delta_ref[i])).astype(BF16)
                dv_s[i, here, :] += _dot(p.astype(BF16), do_ref[i], 1, 0)
                dk_s[i, here, :] += _dot(ds, q_ref[i], 1, 0)
                dq_s[i] += _dot(k_ref[i, here, :].T, ds, 1, 0)

        lax.fori_loop(0, iq, lambda j, _: block(j, False), None)
        block(iq, True)

        def turned_back(wide, at):
            wide = wide.astype(BF16).astype(F32)
            return (wide * cos_ref[at, :] - pltpu.roll(wide, HEAD // 2, 1) * sin_ref[at, :]).astype(BF16)

        def spot(j):
            return pl.ds(pl.multiple_of((j ^ s_ref[1]) * CHUNK, CHUNK), CHUNK)

        at = pl.ds(pl.multiple_of(iq * CHUNK, CHUNK), CHUNK)
        for i in range(few):
            g_ref[spot(iq), i * HEAD : (i + 1) * HEAD] = turned_back((dq_s[i] * SCALE).T, at)

        @pl.when(iq == pl.num_programs(0) - 1)
        def _():
            for j in range(SEQ // CHUNK):
                at = pl.ds(j * CHUNK, CHUNK)
                for i in range(few):
                    low = PART + i * HEAD
                    g_ref[spot(j), low : low + HEAD] = turned_back(dk_s[i, at, :] * SCALE, at)
                    low += PART
                    g_ref[spot(j), low : low + HEAD] = dv_s[i, at, :].astype(BF16)

    half = first // few
    queries = pl.BlockSpec((few, CHUNK, HEAD), lambda i, s: (half, i, 0))
    keys = pl.BlockSpec((few, SEQ, HEAD), lambda i, s: (half, 0, 0), pipeline_mode=pl.Buffered(1))
    stats = pl.BlockSpec((few, 1, CHUNK), lambda i, s: (half, 0, i))
    return call(body, s, SEQ // CHUNK, (q, k, v, do, lse, delta, cos, sin), [queries, keys, keys, queries, stats, stats] + [whole(SEQ, HEAD)] * 2,
                [shape(SEQ, 3 * PART)], [whole(SEQ, 3 * PART)], 5 * few * SEQ * SEQ * HEAD,
                scratch=[pltpu.VMEM((few, HEAD, CHUNK), F32), pltpu.VMEM((few, SEQ, HEAD), F32), pltpu.VMEM((few, SEQ, HEAD), F32)])[0]


def project(s, a, ws, cos, sin, turn, keep):
    outs = len(ws)

    def body(s_ref, *refs):
        a_refs, w_refs, (cos_ref, sin_ref), refs, a_s = refs[:4], refs[4 : 4 + 4 * outs], refs[4 + 4 * outs : 6 + 4 * outs], refs[6 + 4 * outs : -1], refs[-1]
        pick(a_refs, a_s)
        parts = [a_s[:, place(s_ref[0], k)] for k in range(4)]
        for r in refs[outs:]:
            for at, k in enumerate(ORDER):
                r[at * ROWS : (at + 1) * ROWS, :] = parts[k].T
        for n in range(outs):
            for half in range(2):
                acc = total(_dot(parts[k], w_refs[4 * n + k][:, half * PART : (half + 1) * PART], 1, 0) for k in range(4))
                for m in range(HEADS // 2):
                    head = acc[:, m * HEAD : (m + 1) * HEAD].astype(BF16)
                    if turn:
                        wide = head.astype(F32)
                        head = (wide * cos_ref[...] + pltpu.roll(wide, HEAD // 2, 1) * sin_ref[...]).astype(BF16)
                    refs[n][half * (HEADS // 2) + m] = head

    table = pl.BlockSpec((CHUNK, HEAD), lambda i, s: (s[1] ^ i, 0))
    return call(body, s, SEQ // CHUNK, (*a, *(p for w in ws for p in w), cos, sin), [whole(CHUNK, D)] * 4 + [whole(ROWS, D)] * (4 * outs) + [table, table],
                [shape(HEADS, SEQ, HEAD)] * outs + [shape(D, SEQ)] * keep,
                [pl.BlockSpec((HEADS, CHUNK, HEAD), lambda i, s: (0, s[1] ^ i, 0))] * outs + [across()] * keep, 2 * SEQ * D * D * outs,
                scratch=[CHUNKED])


def out_project(s, o, w, first, so_far):
    earlier = [] if so_far is None else [so_far]

    def body(s_ref, o_ref, *refs):
        w_refs, (keep_ref, give_ref, kept) = refs[:4], refs[-3:]
        terms = []
        for at, k in enumerate(ORDER):
            n = 2 * (s_ref[0] ^ k)
            part = jnp.concatenate([o_ref[n], o_ref[n + 1]], axis=1)
            kept[at * ROWS : (at + 1) * ROWS, :] = part.T
            terms.append(_dot(part, w_refs[k][...], 1, 0))
        sort(total(terms).astype(BF16), keep_ref, give_ref)

    return call(body, s, 2, (o, *w, *earlier),
                [pl.BlockSpec((HEADS, CHUNK, HEAD), lambda i, s: (0, s[1] ^ (first + i), 0))] + [whole(ROWS, D)] * 4
                + [pl.BlockSpec(memory_space=pl.ANY)] * len(earlier),
                [shape(CHUNK, D)] * 2 + [shape(D, SEQ)], [TURNS] * 2 + [across(first)], 2 * 2 * CHUNK * D * D,
                aliases={6: 2} if earlier else None)


def heads_back(s, dr, w, o):
    def body(s_ref, *refs):
        o_ref, w_refs, (do_ref, delta_ref, kept) = refs[4], refs[5:9], refs[9:]
        pick(refs[:4], kept)
        for k in range(4):
            pair = _dot(kept[...], w_refs[k][...], 1, 1).astype(BF16)
            for m in range(2):
                do_ref[2 * (s_ref[0] ^ k) + m] = pair[:, m * HEAD : (m + 1) * HEAD]
        for n in range(HEADS):
            delta_ref[n] = (do_ref[n].astype(F32) * o_ref[n].astype(F32)).T.sum(axis=0, keepdims=True)

    heads = pl.BlockSpec((HEADS, CHUNK, HEAD), lambda i, s: (0, s[1] ^ i, 0))
    return call(body, s, SEQ // CHUNK, (*dr, o, *w), [whole(CHUNK, D)] * 4 + [heads] + [whole(ROWS, D)] * 4,
                [shape(HEADS, SEQ, HEAD), shape(HEADS, 1, SEQ, dtype=F32), shape(SEQ, D)],
                [heads, pl.BlockSpec((HEADS, 1, CHUNK), lambda i, s: (0, 0, s[1] ^ i)), rows(D)], 2 * SEQ * D * D)


def project_back(s, g0, g1, ws, first):
    def body(s_ref, g0_ref, g1_ref, *refs):
        w_refs, (keep_ref, give_ref, da_ref) = refs[:12], refs[12:]
        for k in range(4):
            terms = []
            for n, g in enumerate((g0_ref, g1_ref)):
                terms += [_dot(g[:, m * PART : (m + 1) * PART], w_refs[4 * m + k][:, n * PART : (n + 1) * PART], 1, 1) for m in range(3)]
            da_ref[:, place(s_ref[0], k)] = total(terms).astype(BF16)
        sort(da_ref[...], keep_ref, give_ref)

    return call(body, s, 2, (g0, g1, *(p for w in ws for p in w)), [rows(3 * PART, first)] * 2 + [whole(ROWS, D)] * 12,
                [shape(CHUNK, D)] * 2, [TURNS] * 2, 3 * 2 * 2 * CHUNK * D * D, scratch=[CHUNKED])


def hidden_units(s, b, dy, units, down, first, so_far):
    earlier = () if so_far is None else tuple(so_far)
    keep = isinstance(dy, list)
    count = len(b) if keep else dy
    given = (*b, *dy) if keep else b

    def body(s_ref, *refs):
        sources, (w0, w1, w2, w3, down_ref), refs = refs[: len(given)], refs[len(given) : len(given) + 5], refs[len(given) + 5 + len(earlier) :]
        values, dgate_ref, dup_ref = refs[:3]
        if keep:
            b_ref, turned, dy_ref, b_s = refs[3:]
            pick(sources[:count], b_s)
            pick(sources[count:], dy_ref)
            for at, k in enumerate(ORDER):
                part = b_s[:, place(s_ref[0], k)]
                b_ref[:, at * ROWS : (at + 1) * ROWS] = part
                turned[at * ROWS : (at + 1) * ROWS, :] = part.T
        else:
            b_ref, dy_ref = sources
        parts = [(b_ref[:, at * ROWS : (at + 1) * ROWS], (w0, w1, w2, w3)[k]) for at, k in enumerate(ORDER)]
        for c in range(0, D, ROWS):
            g, u = (total(_dot(part, w[:, c + at : c + at + ROWS], 1, 0) for part, w in parts) for at in (0, D))
            dv = _dot(dy_ref[...], down_ref[c : c + ROWS, :], 1, 1).astype(BF16).astype(F32)
            sig = 1.0 / (1.0 + jnp.exp(-g))
            silu = g * sig
            here = slice(c, c + ROWS)
            values[here, :] = (silu * u).astype(BF16).T
            dup_ref[:, here] = (dv * silu).astype(BF16)
            dgate_ref[:, here] = (dv * u * (sig + silu * (1.0 - sig))).astype(BF16)

    wide, tall = shape(2 * SEQ, D), shape(D, 2 * SEQ)
    return call(body, s, count, (*given, *units, down, *earlier),
                ([whole(CHUNK, D)] * len(given) if keep else [rows(D, first)] * 2) + [whole(ROWS, 2 * D)] * 4 + [whole(D, D)]
                + [pl.BlockSpec(memory_space=pl.ANY)] * len(earlier),
                [tall, wide, wide] + [wide, tall, wide] * keep, [across(first)] + [rows(D, first)] * 2 + [rows(D, first), across(first), rows(D, first)] * keep,
                6 * count * CHUNK * D * D, aliases={len(given) + 6 + i: i for i in range(len(earlier))}, scratch=[CHUNKED] * keep)


def hidden_back(s, grads, units, first):
    def body(s_ref, *refs):
        for k in range(4):
            terms = []
            for n in range(4):
                w = refs[4 + n // 2 * 4 + k]
                terms.append(_dot(refs[n][...], w[:, n % 2 * D : (n % 2 + 1) * D], 1, 1))
            refs[-1][:, place(s_ref[0], k)] = total(terms).astype(BF16)
        sort(refs[-1][...], refs[-3], refs[-2])

    return call(body, s, 4, (*grads, *units[0], *units[1]), [rows(D, first)] * 4 + [whole(ROWS, 2 * D)] * 8,
                [shape(2 * CHUNK, D)] * 2, [TURNS] * 2, 4 * SEQ * D * 2 * D, scratch=[CHUNKED])


def by_weight(s, a, blocks, gs, tile, more=None, swap=False, split=False, placed=False):
    tokens, height = a.shape[1], len(blocks) * ROWS
    steps = [n // tile for _, _, n in gs]
    n_tiles = sum(steps)
    joined = all(b == blocks[0] + i for i, b in enumerate(blocks)) and blocks[0] % len(blocks) == 0
    a_specs = ([pl.BlockSpec((height, tokens), lambda i, s: (blocks[0] // len(blocks), 0), pipeline_mode=pl.Buffered(1))] if joined
               else [pl.BlockSpec((ROWS, tokens), lambda i, s, b=b: (b, 0), pipeline_mode=pl.Buffered(1)) for b in blocks])

    def body(s_ref, *refs):
        a_refs, g_refs, rest = refs[: len(a_specs)], refs[len(a_specs) : len(a_specs) + len(gs)], refs[len(a_specs) + len(gs) :]
        low = 0
        for g, n in zip(g_refs, steps):

            @pl.when((pl.program_id(0) >= low) & (pl.program_id(0) < low + n))
            def _():
                lhs = a_refs[0][...] if joined else jnp.concatenate([r[...] for r in a_refs], axis=0)
                acc = _dot(lhs, g[...], 1, 0)
                if more is not None:
                    extra = rest[0][...].astype(F32)
                    acc = acc + (jnp.concatenate([extra[ROWS:], extra[:ROWS]], axis=0) if swap else extra)
                if split:
                    rest[-2][...] = acc[:ROWS].astype(BF16)
                    rest[-1][...] = acc[ROWS:].astype(BF16)
                else:
                    rest[-1][...] = acc.astype(BF16)

            low += n

    def run(i, s):
        return (i // steps[0] ^ s[2]) * steps[0] + i % steps[0] if placed else i

    g_specs, low = [], 0
    for (_, start, _), n in zip(gs, steps):
        g_specs.append(pl.BlockSpec((tokens, tile), lambda i, s, low=low, n=n, start=start: (0, start // tile + jnp.clip(i - low, 0, n - 1))))
        low += n
    extra = [] if more is None else [more]
    width = n_tiles * tile
    if split:
        outs = [shape(ROWS, width * (1 + placed)), shape(ROWS, width)]
        specs = [pl.BlockSpec((ROWS, tile), lambda i, s: (0, (s[0] // 2 * n_tiles if placed else 0) + run(i, s))),
                 pl.BlockSpec((ROWS, tile), lambda i, s: (0, run(i, s)))]
    else:
        outs, specs = [shape(height, width)], [pl.BlockSpec((height, tile), lambda i, s: (0, i))]
    got = call(body, s, n_tiles, (*[a] * len(a_specs), *(g for g, _, _ in gs), *extra),
               a_specs + g_specs + [pl.BlockSpec((height, tile), lambda i, s: (0, i))] * len(extra), outs, specs, 2 * tokens * height * width)
    return got if split else got[0]


def solution(mesh):
    def flip(v, axis, bit):
        return lax.ppermute(v, axis, [(i, i ^ bit) for i in range(4)])

    def over_core(v):
        return flip(v, "tp", 1)

    def over_x(v):
        return flip(v, "tp", 2)

    def over_z(v):
        return flip(v, "dp", 1)

    def over_y(v):
        return flip(v, "dp", 2)

    def normed(h):
        wide = h.astype(F32)
        scale = lax.rsqrt(jnp.mean(wide**2, -1, keepdims=True) + 1e-6)
        return (wide * scale).astype(BF16)

    def added(*terms):
        return sum(t.astype(F32) for t in terms).astype(BF16)

    def step(x, dy, wq, wk, wv, wo, w_gate, w_up, w_down):
        d, t = lax.axis_index("dp"), lax.axis_index("tp")
        y, z = d // 2, d % 2
        s = jnp.stack([d, t, z]).astype(jnp.int32)
        x, dy = x[0], dy[0]

        a = normed(x)
        ax = over_x(a)
        a_all = [a, over_core(a), ax, over_core(ax)]
        q_z, k_y = over_z(wq), over_y(wk)
        wqs = wq, q_z, over_y(wq), over_y(q_z)
        wks = wk, over_z(wk), k_y, over_z(k_y)
        wvs = wv, over_z(wv), over_y(wv), flip(wv, "dp", 3)
        wo_z = over_z(wo)
        wos = wo, wo_z, over_y(wo), over_y(wo_z)

        dyx, dyy = over_x(dy), over_y(dy)
        dyyx = over_x(dyy)
        dy_own = [dy, over_core(dy)]
        dy_near = [dyx, over_core(dyx), dyy, over_core(dyy)]
        dy_far = [dyyx, over_core(dyyx)]

        def run(r):
            return jnp.concatenate([lax.dynamic_slice_in_dim(w, r * D, D, axis=1) for w in (w_gate, w_up)], axis=1)

        m0, m1 = run(d), run(d ^ 1)
        f0, f1 = over_y(run(d ^ 2)), over_y(run(d ^ 3))
        first = m0, over_z(m1), f0, over_z(f1)
        second = m1, over_z(m0), f1, over_z(f0)
        down_z = over_z(w_down)

        half = HEAD // 2
        angle = jnp.arange(SEQ, dtype=F32)[:, None] * THETA ** (-jnp.arange(half, dtype=F32) / half)
        cos = jnp.concatenate([jnp.cos(angle)] * 2, axis=1)
        sin = jnp.concatenate([-jnp.sin(angle), jnp.sin(angle)], axis=1)

        q, k, a_rows = project(s, a_all, (wqs, wks), cos, sin, True, 1)
        v = project(s, a_all, (wvs,), cos, sin, False, 0)[0]
        o, lse = attend(s, q, k, v)
        keep, give, o_rows = out_project(s, o, wos, 2, None)
        rx = over_x(added(keep, over_core(give)))
        keep, give, o_rows = out_project(s, o, wos, 0, o_rows)
        h = x + added(keep, over_core(give), rx)

        b = normed(h)
        bx, by = over_x(b), over_y(b)
        byx = over_x(by)
        b_own = [b, over_core(b)]
        b_near = [bx, over_core(bx), by, over_core(by)]
        b_far = [byx, over_core(byx)]
        got = hidden_units(s, b_own, dy_own, first, w_down, 0, None)
        got = hidden_units(s, b_near, dy_near, first, w_down, 2, got)
        got2 = hidden_units(s, (got[3], got[5]), 6, second, down_z, 0, None)
        got = hidden_units(s, b_far, dy_far, first, w_down, 6, got)
        values, dgate, dup, b_cols, b_rows, dys = got
        values2, dgate2, dup2 = hidden_units(s, (b_cols, dys), 2, second, down_z, 6, got2)

        grads = dgate, dup, dgate2, dup2
        keep, give = hidden_back(s, grads, (first, second), 4)
        other = over_core(give)
        fx = over_x(added(keep[CHUNK:], other[CHUNK:]))
        fy = over_y(added(keep[:CHUNK], other[:CHUNK], fx))
        keep, give = hidden_back(s, grads, (first, second), 0)
        other = over_core(give)
        nx = over_x(added(keep[CHUNK:], other[CHUNK:]))
        db = added(keep[:CHUNK], other[:CHUNK], nx, fy)
        dh = dy + jax.vjp(normed, h)[1](db)[0]

        everything = range(D // ROWS)
        away = over_z(by_weight(s, values2, everything, [(dys, 0, D)], CHUNK))
        by_down = by_weight(s, values, everything, [(dys, 0, D)], CHUNK, away)

        def by_units(g0, g1):
            away = over_z(by_weight(s, b_rows, (2, 3), [(g1, 0, D), (g0, 0, D)], CHUNK))
            kept, going = by_weight(s, b_rows, (0, 1), [(g0, 0, D), (g1, 0, D)], CHUNK, away, True, True, True)
            from_y = over_y(going)
            return lax.dynamic_update_slice_in_dim(kept, from_y, (1 - y) * 2 * D, axis=1)

        by_gate, by_up = by_units(dgate, dgate2), by_units(dup, dup2)

        def scattered(a, g):
            n = g.shape[1] // 2
            g0, g1 = [(g, 0, n)], [(g, n, n)]
            got = over_z(by_weight(s, a, (2, 3), g0, ROWS))
            got1 = over_y(by_weight(s, a, (1, 2), g1, ROWS))
            here, going = by_weight(s, a, (0, 1), g0, ROWS, got, True, True)
            here1, going1 = by_weight(s, a, (0, 3), g1, ROWS, got1, False, True)
            last, last1 = over_y(going), over_z(going1)
            return jnp.concatenate([added(here, last), added(here1, last1)], axis=1)

        dhx = over_x(dh)
        dr = [dh, over_core(dh), dhx, over_core(dhx)]
        do, delta, dr = heads_back(s, dr, wos, o)
        by_o = scattered(o_rows, dr)
        g0 = attend_back(s, q, k, v, do, lse, delta, cos, sin, 0)
        part0 = scattered(a_rows, g0)
        g1 = attend_back(s, q, k, v, do, lse, delta, cos, sin, HEADS // 2)
        keep, give = project_back(s, g0, g1, (wqs, wks, wvs), 2)
        got = over_x(added(keep, over_core(give)))
        part1 = scattered(a_rows, g1)
        keep, give = project_back(s, g0, g1, (wqs, wks, wvs), 0)
        da = added(keep, over_core(give), got)
        by_x = dh + jax.vjp(normed, x)[1](da)[0]
        by_q, by_k, by_v = (jnp.concatenate([p[:, i : i + PART] for p in (part0, part1)], axis=1) for i in range(0, 3 * PART, PART))
        return (by_x[None], by_q, by_k, by_v, by_o, by_gate, by_up, by_down)

    states, by_columns, by_rows = P("dp", "tp", None), P("dp", "tp"), P(("tp", "dp"), None)
    weights = (by_columns, by_columns, by_columns, by_rows, by_columns, by_columns, by_rows)
    return jax.shard_map(step, mesh=mesh, in_specs=(states, states, *weights), out_specs=(states, *weights), check_vma=False)
```
